512 devices in a mesh: scen: 2 (over y), row: 32 (over z), col: 4 (over x), layer: 2 (over core).
Axes of the slice: x: 4, y: 2, z: 32, core: 2. Of those that a mesh axis runs over, the one named last changes fastest.
The devices are a block of a 4x8x32 slice.
Arguments:
- current: float32 [2, 8192, 4096], P('layer', ('scen', 'row'), 'col'), parts along dimension 1, may hold values from 0.5 to 10
- node_class: int32 [2, 8192, 4096], P('layer', ('scen', 'row'), 'col'), parts along dimension 1, may hold values from 0 to 7
- class_conductance: float32 [2, 8], P('layer'), may hold values from 0.5 to 4
- pad_mask: int32 [2, 8192, 4096], P('layer', ('scen', 'row'), 'col'), parts along dimension 1, may hold values 0 or 1
- via_mask: int32 [8192, 4096], P(('scen', 'row'), 'col'), parts along dimension 0, may hold values 0 or 1
Outputs:
- drop: float32 [2, 8192, 4096], P('layer', ('scen', 'row'), 'col'), parts along dimension 1
- residual: float32 [2, 8192, 4096], P('layer', ('scen', 'row'), 'col'), parts along dimension 1
- worst: float32 [2, 8192, 4096], P('layer', ('scen', 'row'), 'col'), parts along dimension 1
The draws below stay inside these ranges and needn't reach their ends.
There are 2 independent parts, one for each index of `scen`. The reference program is written for one: setup_inputs(seed, part) draws one part's arguments, and reference() takes and returns one part's arrays. A program takes and returns all parts, laid end to end along the dimension named above; an argument that names none is the same for every part. Nothing has to cross between parts.
All inputs are finite; a program needn't handle non-finite values. No bound on the sum of `pad_mask` or of `via_mask` on one device may be relied on, other than what follows from the above.
Results may differ from the reference program's by a relative error of at most 0.0003.
Values sent between devices are 32-bit elements; how exact they have to be, the bound alone decides.
No kernel may reach another device: no remote copies, remote signals or barrier semaphores. Data moves between devices by JAX's collectives and lax.ppermute only.
A program may use at most 64 MiB of HBM per device.

```python
import math
import jax
import jax.numpy as jnp

CLASSES = 8
ITERS = 2
NX = 4096
NY = 4096
LAYERS = 2


def with_ends(entries, stream_key, smallest, high):
    spot = [jax.random.randint(jax.random.fold_in(stream_key, axis), (), 0, length) for axis, length in enumerate(entries.shape)]
    longest = entries.shape.index(max(entries.shape))
    next_to = spot[:longest] + [(spot[longest] + 1) % entries.shape[longest]] + spot[longest + 1:]
    return entries.at[tuple(spot)].set(smallest).at[tuple(next_to)].set(high)


def shard_levels(rng, shape, shards, low, high):
    def one(position, shards_of):
        steps = jax.random.uniform(jax.random.fold_in(jax.random.fold_in(rng, 6), position), (shards_of,), jnp.float32, low / len(shards), high / len(shards))
        return jnp.repeat(jnp.exp(steps), shape[position] // shards_of).reshape((-1,) + (1,) * (len(shape) - position - 1))

    gain = one(*shards[0])
    for cut in shards[1:]:
        gain = gain * one(*cut)
    return gain


def setup_inputs(seed: int = 0, part: int = 0) -> dict:
    streams_of = jax.random.split(jax.random.key(seed), 6)
    own_keys = jax.random.split(jax.random.fold_in(streams_of[5], part), 6)
    return {
        "current": jnp.clip(jnp.exp(math.log(10.0) - 2.9957323 * jax.random.uniform(own_keys[0], (LAYERS, NX, NY), jnp.float32) ** shard_levels(own_keys[0], (LAYERS, NX, NY), ((0, 2), (1, 32), (2, 4)), -0.2, 0.2)), 0.5, 10.0),
        "node_class": with_ends(jax.random.randint(own_keys[1], (LAYERS, NX, NY), 0, CLASSES), jax.random.fold_in(own_keys[1], 1), 0, CLASSES - 1).astype(jnp.int32),
        "class_conductance": jnp.clip(jnp.exp(math.log(4.0) - 2.0794415 * jax.random.uniform(streams_of[2], (LAYERS, CLASSES), jnp.float32) ** shard_levels(streams_of[2], (LAYERS, CLASSES), ((0, 2),), -0.2, 0.2)), 0.5, 4.0),
        "pad_mask": with_ends((jax.random.randint(own_keys[3], (LAYERS, NX, NY), 0, 16) < 1).astype(jnp.int32), jax.random.fold_in(own_keys[3], 1), 0, 1),
        "via_mask": with_ends((jax.random.randint(own_keys[4], (NX, NY), 0, 2) < 1).astype(jnp.int32), jax.random.fold_in(own_keys[4], 1), 0, 1),
    }


via_conductance = 2.0
pad_conductance = 4.0
leakage = 0.05


def lookup(node_class, class_conductance):
    cond = jnp.zeros(node_class.shape, jnp.float32)
    for klass in range(class_conductance.shape[1]):
        cond = cond + jnp.where(node_class == klass, class_conductance[:, klass][:, None, None], jnp.float32(0.0))
    return cond


def edge_terms(cond):
    padded = jnp.pad(cond, ((0, 0), (1, 1), (1, 1)))
    beside_all = (padded[:, :-2, 1:-1], padded[:, 2:, 1:-1], padded[:, 1:-1, :-2], padded[:, 1:-1, 2:])
    return tuple(jnp.where(other > 0.0, 0.5 * (cond + other), jnp.float32(0.0)) for other in beside_all)


def apply_grid(values, edges, diagonal, coupling):
    padded = jnp.pad(values, ((0, 0), (1, 1), (1, 1)))
    beside = edges[0] * padded[:, :-2, 1:-1] + edges[1] * padded[:, 2:, 1:-1]
    beside = beside + edges[2] * padded[:, 1:-1, :-2] + edges[3] * padded[:, 1:-1, 2:]
    return diagonal * values - beside - coupling * values[::-1]


def reference(current, node_class, class_conductance, pad_mask, via_mask):
    cond = lookup(node_class, class_conductance)
    edges = edge_terms(cond)
    coupling = via_conductance * via_mask.astype(jnp.float32)
    diagonal = edges[0] + edges[1] + edges[2] + edges[3] + coupling + pad_conductance * pad_mask.astype(jnp.float32) + leakage
    drop_field = jnp.zeros_like(current)
    resid = current
    precond = resid / diagonal
    direction = precond
    energy_now = jnp.sum(resid * precond)
    worst_field = drop_field
    for iteration in range(ITERS):
        image = apply_grid(direction, edges, diagonal, coupling)
        step_size = energy_now / jnp.sum(direction * image)
        drop_field = drop_field + step_size * direction
        resid = resid - step_size * image
        worst_field = drop_field if iteration == 0 else jnp.maximum(worst_field, drop_field)
        if iteration + 1 < ITERS:
            precond = resid / diagonal
            energy_next = jnp.sum(resid * precond)
            direction = precond + (energy_next / energy_now) * direction
            energy_now = energy_next
    return drop_field, resid, worst_field
```

```python
import jax
import jax.numpy as jnp
from jax import lax
from jax.sharding import PartitionSpec as P

via_conductance = 2.0
pad_conductance = 4.0
leakage = 0.05


def with_halo(value, sides, width):
    edges = {}
    for axis, dim in sides:
        size, length = (lax.axis_size(axis), value.shape[dim])
        up = [(i, (i + 1) % size) for i in range(size - 1)]
        last = lax.slice_in_dim(value, length - width, length, axis=dim)
        initial = lax.slice_in_dim(value, 0, width, axis=dim)
        edges[dim] = (
            lax.ppermute(last, axis, up),
            lax.ppermute(initial, axis, [(b, a) for a, b in up]),
        )
    done = []
    for _, dim in sides:
        low, high = edges[dim]
        around = [(width, width) if d in done else (0, 0) for d in range(value.ndim)]
        value = jnp.concatenate([jnp.pad(low, around), value, jnp.pad(high, around)], axis=dim)
        done.append(dim)
    return value


def from_partner(value, axis, stride):
    return lax.ppermute(value, axis, [(i, i ^ 1 << stride) for i in range(lax.axis_size(axis))])


def global_sums(fields):
    axes = ("row", "col", "layer")
    count = 1
    for axis in axes:
        count *= lax.axis_size(axis)
    parts = jnp.stack([jnp.sum(field) for field in fields])
    sent = jnp.broadcast_to(parts[None, None, :], (count, 1, parts.shape[0]))
    return jnp.sum(lax.all_to_all(sent, axes, 0, 0, tiled=True), axis=(0, 1))


def lookup(node_class, class_conductance):
    cond = jnp.zeros(node_class.shape, jnp.float32)
    for klass in range(class_conductance.shape[1]):
        cond = cond + jnp.where(
            node_class == klass, class_conductance[:, klass][:, None, None], jnp.float32(0.0)
        )
    return cond


def edge_terms(cond):
    padded = with_halo(cond, (("row", 1), ("col", 2)), 1)
    beside_all = (
        padded[:, :-2, 1:-1],
        padded[:, 2:, 1:-1],
        padded[:, 1:-1, :-2],
        padded[:, 1:-1, 2:],
    )
    return tuple(
        (jnp.where(other > 0.0, 0.5 * (cond + other), jnp.float32(0.0)) for other in beside_all)
    )


def apply_grid(values, edges, diagonal, coupling):
    padded = with_halo(values, (("row", 1), ("col", 2)), 1)
    partner = from_partner(values, "layer", 0)
    beside = edges[0] * padded[:, :-2, 1:-1] + edges[1] * padded[:, 2:, 1:-1]
    beside = beside + edges[2] * padded[:, 1:-1, :-2] + edges[3] * padded[:, 1:-1, 2:]
    return diagonal * values - beside - coupling * partner


def local(current, node_class, class_conductance, pad_mask, via_mask):
    cond = lookup(node_class, class_conductance)
    edges = edge_terms(cond)
    coupling = via_conductance * via_mask.astype(jnp.float32)
    diagonal = (
        edges[0]
        + edges[1]
        + edges[2]
        + edges[3]
        + coupling
        + pad_conductance * pad_mask.astype(jnp.float32)
        + leakage
    )
    scaled = current / diagonal
    image = apply_grid(scaled, edges, diagonal, coupling)
    second = image / diagonal
    second_image = apply_grid(second, edges, diagonal, coupling)
    sums = global_sums(
        (current * scaled, scaled * image, image * second, second * second_image)
    )
    energy, curve, cross, last = sums[0], sums[1], sums[2], sums[3]
    step = energy / curve
    energy_next = step * step * cross - energy
    ratio = energy_next / energy
    curve_next = curve - 2.0 * step * cross + step * step * last - ratio * ratio * curve
    step_next = energy_next / curve_next
    first_drop = step * scaled
    direction = (1.0 + ratio) * scaled - step * second
    along = (1.0 + ratio) * image - step * second_image
    drop_field = first_drop + step_next * direction
    resid = current - step * image - step_next * along
    return (drop_field, resid, jnp.maximum(first_drop, drop_field))


def solution(mesh):
    in_specs = (
        P("layer", ("scen", "row"), "col"),
        P("layer", ("scen", "row"), "col"),
        P("layer", None),
        P("layer", ("scen", "row"), "col"),
        P(("scen", "row"), "col"),
    )
    out_specs = (
        P("layer", ("scen", "row"), "col"),
        P("layer", ("scen", "row"), "col"),
        P("layer", ("scen", "row"), "col"),
    )
    return jax.shard_map(local, mesh=mesh, in_specs=in_specs, out_specs=out_specs, check_vma=False)
```

```python
import functools

import jax
import jax.numpy as jnp
from jax import lax
from jax.experimental import pallas as pl
from jax.experimental.pallas import tpu as pltpu
from jax.sharding import PartitionSpec as P

via_conductance = 2.0
pad_conductance = 4.0
leakage = 0.05

SUB = 8
LANE = 128


def lanes_of(shape):
    return lax.broadcasted_iota(jnp.int32, shape, len(shape) - 1)


def rows_of(shape):
    return lax.broadcasted_iota(jnp.int32, shape, len(shape) - 2)


def turned(value, shift, axis):
    size = value.shape[axis]
    return pltpu.roll(value, shift % size, axis) if shift % size else value


def conductance(classes, table):
    cond = jnp.zeros(classes.shape, jnp.float32)
    for klass in range(table.shape[1]):
        cond = jnp.where(classes == klass, table[0, klass], cond)
    return cond


def pad_term(pads):
    return pad_conductance * pads.astype(jnp.float32) + leakage


def via_term(vias):
    return via_conductance * vias.astype(jnp.float32)


def border_rows(table, top, bottom):
    out = []
    for blocks, shifts, far in ((top, (0, 3, 5, 7), 1), (bottom, (3, 5, 7, 0), SUB - 2)):
        classes, current, pads, vias = blocks
        row = rows_of(current.shape)
        cond = conductance(classes, table)
        coupling = via_term(vias)
        own = pad_term(pads)
        own = jnp.where(row == far, own + coupling, own)
        parts = [turned(v, s, 0) for v, s in zip((cond, current, own, coupling), shifts)]
        out.append(
            jnp.where(row < 3, parts[0], jnp.where(row < 5, parts[1], jnp.where(row < 7, parts[2], parts[3])))
        )
    return out


def rows_kernel(table, ct, rt, pt, vt, cb, rb, pb, vb, up, down):
    up[...], down[...] = border_rows(
        table, (ct[0], rt[0], pt[0], vt[...]), (cb[0], rb[0], pb[0], vb[...])
    )


def border_columns(low, high):
    lane = lanes_of(low[0].shape)
    out = None
    for blocks, shifts, far, start in ((high, (3, 5, 7, 8), LANE - 2, 0), (low, (8, 11, 13, 15), 1, 8)):
        cond, current, own, coupling = blocks
        own = jnp.where(lane == far, own + coupling, own)
        parts = [turned(v, s, 1) for v, s in zip((cond, current, own, coupling), shifts)]
        at = lane - start
        side = jnp.where(at < 3, parts[0], jnp.where(at < 5, parts[1], jnp.where(at < 7, parts[2], parts[3])))
        out = side if out is None else jnp.where(lane < start, out, side)
    return out


def tile_kernel(table, classes, current, pads, vias, bulk, strips):
    rows, width = vias.shape

    def strip(s, carry):
        at = pl.ds(pl.multiple_of(s * SUB, SUB), SUB)
        bulk[0, at, :] = conductance(classes[0, at, :], table)
        bulk[1, at, :] = current[0, at, :]
        bulk[2, at, :] = pad_term(pads[0, at, :])
        return carry

    lax.fori_loop(0, rows // SUB, strip, 0)
    sides = [
        (bulk[0, :, at], bulk[1, :, at], bulk[2, :, at], via_term(vias[:, at]))
        for at in (slice(0, LANE), slice(width - LANE, width))
    ]
    strips[...] = border_columns(*sides).T[: 2 * SUB]


def spread_rows(message, below):
    shifts, firsts = ((0, 5, 3, 1), (0, 0, 0, 0)) if below else ((5, 3, 1, 0), (5, 6, 6, 7))
    counts = (3, 2, 2, 1)
    row = rows_of(message.shape)
    return [
        jnp.where((row >= f) & (row < f + n), turned(message, s, 0), 0.0)
        for s, f, n in zip(shifts, firsts, counts)
    ]


def send_kernel(place, top, bottom, strips, send):
    width = top.shape[1]
    blocks = []
    for at in (slice(0, LANE), slice(width - LANE, width)):
        above = spread_rows(top[:, at], False)
        under = spread_rows(bottom[:, at], True)
        blocks.append([jnp.concatenate([a, b], axis=0) for a, b in zip(above, under)])
    around = border_columns(*blocks)
    around = jnp.concatenate([around, jnp.zeros((LANE - 2 * SUB, LANE), jnp.float32)], axis=0).T
    high = jnp.concatenate([strips[:SUB], around[:SUB]], axis=1)
    low = jnp.concatenate([strips[SUB:], around[SUB : 2 * SUB]], axis=1)
    for k in range(send.shape[0]):
        send[k] = jnp.where(k // 2 > place[0], high, low)


def side_lanes(left, right):
    fill = jnp.zeros((LANE - 2 * SUB, LANE), jnp.float32)
    both = jnp.concatenate([left, right, fill], axis=0).T
    lane = lanes_of(both.shape)
    out = []
    for first, before, after in ((0, 3, 3), (3, 2, 2), (5, 2, 2), (7, 1, 1)):
        low = turned(both, LANE - before - first, 1)
        high = turned(both, -SUB - first, 1)
        out.append(jnp.where(lane >= LANE - before, low, jnp.where(lane < after, high, 0.0)))
    return out


def grid_kernel(
    place, own, other, vias, top, bottom, frames, recv,
    z_out, u_out, w_out, v_out, sums,
    cond, resid, extra, coup, eh, ev, inv, z, u, flux,
):
    rows, width = vias.shape
    strips = rows // SUB
    wide = width + LANE
    columns = recv.shape[0] // 2

    def at(s):
        return pl.ds(pl.multiple_of((s + 1) * SUB, SUB), SUB)

    for layer in range(2):
        source = own if layer == 0 else other
        mine = place[1] if layer == 0 else 1 - place[1]
        c = place[0]
        left = recv[jnp.maximum(2 * (c - 1) + mine, 0)]
        left = jnp.where(c > 0, left, 0.0)
        right = recv[jnp.minimum(2 * (c + 1) + mine, 2 * columns - 1)]
        right = jnp.where(c < columns - 1, right, 0.0)
        beside = side_lanes(left[:, :LANE], right[:, :LANE])
        corner = side_lanes(left[:, LANE:], right[:, LANE:])
        above = spread_rows(top[...] if layer == 0 else frames[:SUB], False)
        under = spread_rows(bottom[...] if layer == 0 else frames[SUB:], True)
        fields = [cond, resid, extra] + ([coup] if layer == 0 else [])
        for k, field in enumerate(fields):
            to = field.at[layer] if k < 3 else field
            to[SUB : 2 * SUB, :width] = above[k]
            to[(strips + 2) * SUB : (strips + 3) * SUB, :width] = under[k]
            to[SUB : 2 * SUB, width:] = corner[k][:SUB]
            to[(strips + 2) * SUB : (strips + 3) * SUB, width:] = corner[k][SUB : 2 * SUB]
            to[2 * SUB : (strips + 2) * SUB, width:] = beside[k]
            if k < 3:
                to[2 * SUB : (strips + 2) * SUB, :width] = source[k]
            else:
                to[2 * SUB : (strips + 2) * SUB, :width] = via_term(vias[...])

    row = rows_of((SUB, wide))
    first, last = row == 0, row == SUB - 1

    def after(value):
        return turned(value, -1, 1)

    def before(value):
        return turned(value, 1, 1)

    def below(value, following):
        return turned(jnp.where(first, following, value), -1, 0)

    def above_of(value, preceding):
        return turned(jnp.where(last, preceding, value), 1, 0)

    def edge(a, b):
        return jnp.where((a > 0.0) & (b > 0.0), 0.5 * (a + b), 0.0)

    def scale(s, carry):
        k = coup[at(s), :]
        for layer in range(2):
            c = cond[layer, at(s), :]
            h = edge(c, after(c))
            v = edge(c, below(c, cond[layer, at(s + 1), :]))
            eh[layer, at(s), :] = h
            ev[layer, at(s), :] = v
            diagonal = h + before(h) + v + above_of(v, ev[layer, at(s - 1), :]) + k + extra[layer, at(s), :]
            inverse = jnp.where(c > 0.0, 1.0 / diagonal, 0.0)
            inv[layer, at(s), :] = inverse
            z[layer, at(s), :] = resid[layer, at(s), :] * inverse
        return carry

    lax.fori_loop(0, strips + 2, scale, 0)

    def folded(value):
        parts = [value[:, i * LANE : (i + 1) * LANE] for i in range(width // LANE)]
        while len(parts) > 1:
            parts = [a + b for a, b in zip(parts[::2], parts[1::2])]
        return parts[0]

    def image(field, s, layer, k):
        x = field[layer, at(s), :]
        fh = eh[layer, at(s), :] * (x - after(x))
        fv = ev[layer, at(s), :] * (x - below(x, field[layer, at(s + 1), :]))
        previous = flux[layer, at(s - 1), :]
        flux[layer, at(s), :] = fv
        there = field[1 - layer, at(s), :]
        return x, fh - before(fh) + fv - above_of(fv, previous) + k * (x - there) + extra[layer, at(s), :] * x

    def second(s, keep):
        k = coup[at(s), :]
        found = []
        for layer in range(2):
            x, w = image(z, s, layer, k)
            y = w * inv[layer, at(s), :]
            u[layer, at(s), :] = y
            found.append((x, w, y))
        if not keep:
            return None
        to = pl.ds(pl.multiple_of((s - 1) * SUB, SUB), SUB)
        z_out[to, :] = found[0][0][:, :width]
        w_out[to, :] = found[0][1][:, :width]
        u_out[to, :] = found[0][2][:, :width]
        energy = folded(sum(resid[i, at(s), :] * found[i][0] for i in range(2)))
        curve = folded(sum(found[i][0] * found[i][1] for i in range(2)))
        cross = folded(sum(found[i][1] * found[i][2] for i in range(2)))
        return energy, curve, cross

    zero = jnp.zeros((SUB, LANE), jnp.float32)
    second(0, False)
    totals = lax.fori_loop(
        1, strips + 1, lambda s, t: tuple(a + b for a, b in zip(t, second(s, True))), (zero,) * 3
    )
    second(strips + 1, False)

    x = u[0, at(0), :]
    flux[0, at(0), :] = ev[0, at(0), :] * (x - below(x, u[0, at(1), :]))

    def third(s, total):
        k = coup[at(s), :]
        x, v = image(u, s, 0, k)
        to = pl.ds(pl.multiple_of((s - 1) * SUB, SUB), SUB)
        v_out[to, :] = v[:, :width]
        y = u[1, at(s), :]
        dh = y - after(y)
        dv = y - below(y, u[1, at(s + 1), :])
        there = eh[1, at(s), :] * dh * dh + ev[1, at(s), :] * dv * dv
        there = there + y * (k * (y - x) + extra[1, at(s), :] * y)
        return total + folded(x * v + there)

    total = lax.fori_loop(1, strips + 1, third, zero)
    lane = lanes_of((1, LANE))
    line = jnp.zeros((1, LANE), jnp.float32)
    for k, value in enumerate(totals + (total,)):
        line = jnp.where(lane == k, jnp.sum(value, axis=(0, 1), keepdims=True), line)
    sums[...] = jnp.broadcast_to(line[None], sums.shape)


def finish_kernel(parts, current, z, u, w, v, drop, resid, worst):
    line = jnp.sum(parts[...], axis=0)
    lane = lanes_of(line.shape)
    energy, curve, cross, last = (
        jnp.sum(jnp.where(lane == k, line, 0.0), axis=1, keepdims=True) for k in range(4)
    )
    step = energy / curve
    energy_next = step * step * cross - energy
    ratio = energy_next / energy
    curve_next = curve - 2.0 * step * cross + step * step * last - ratio * ratio * curve
    step_next = energy_next / curve_next
    keep = 1.0 + ratio
    first_drop = step * z[...]
    second_drop = first_drop + step_next * (keep * z[...] - step * u[...])
    drop[0] = second_drop
    worst[0] = jnp.maximum(first_drop, second_drop)
    resid[0] = current[0] - step * w[...] - step_next * (keep * w[...] - step * v[...])


def local(current, node_class, class_conductance, pad_mask, via_mask):
    _, rows, width = current.shape
    n_row, n_col = lax.axis_size("row"), lax.axis_size("col")
    up_pairs = [(i, i + 1) for i in range(n_row - 1)]
    down_pairs = [(b, a) for a, b in up_pairs]
    swap = [(0, 1), (1, 0)]
    place = jnp.stack([lax.axis_index("col"), lax.axis_index("layer")]).astype(jnp.int32)
    f32 = jnp.float32
    smem = pl.BlockSpec(memory_space=pltpu.SMEM)
    vmem = pl.BlockSpec(memory_space=pltpu.VMEM)

    def shape(*dims):
        return jax.ShapeDtypeStruct(dims, f32)

    def ends(index):
        block = pl.BlockSpec((1, SUB, width), lambda i: (0, index, 0))
        return [block] * 3 + [pl.BlockSpec((SUB, width), lambda i: (index, 0))]

    fields = (node_class, current, pad_mask, via_mask)
    message = pl.BlockSpec((SUB, width), lambda i: (0, 0))
    up, down = pl.pallas_call(
        rows_kernel,
        grid=(1,),
        in_specs=[smem] + ends(0) + ends(rows // SUB - 1),
        out_specs=[message] * 2,
        out_shape=[shape(SUB, width)] * 2,
        name="border_rows",
    )(class_conductance, *fields, *fields)
    top = lax.ppermute(down, "row", up_pairs)
    bottom = lax.ppermute(up, "row", down_pairs)

    bulk, strips = pl.pallas_call(
        tile_kernel,
        in_specs=[smem] + [vmem] * 4,
        out_specs=[vmem] * 2,
        out_shape=[shape(3, rows, width), shape(2 * SUB, LANE)],
        name="tile_fields",
    )(class_conductance, *fields)
    other = lax.ppermute(bulk, "layer", swap)

    frames = lax.ppermute(jnp.concatenate([top, bottom], axis=0), "layer", swap)
    send = pl.pallas_call(
        send_kernel,
        in_specs=[smem] + [vmem] * 3,
        out_specs=vmem,
        out_shape=shape(2 * n_col, SUB, 2 * LANE),
        name="border_columns",
    )(place, top, bottom, strips)
    recv = lax.all_to_all(send, ("col", "layer"), 0, 0, tiled=True)

    full = (rows + 4 * SUB, width + LANE)
    pair = pltpu.VMEM((2,) + full, f32)
    z, u, w, v, sums = pl.pallas_call(
        grid_kernel,
        in_specs=[smem] + [vmem] * 7,
        out_specs=[vmem] * 5,
        out_shape=[shape(rows, width)] * 4 + [shape(n_row * n_col, 1, LANE)],
        scratch_shapes=[pair, pair, pair, pltpu.VMEM(full, f32)] + [pair] * 6,
        name="grid",
    )(place, bulk, other, via_mask, top, bottom, frames, recv)
    parts = lax.all_to_all(sums, ("row", "col"), 0, 0, tiled=True)

    pieces = 4
    part = rows // pieces
    flat = pl.BlockSpec((part, width), lambda i: (i, 0))
    deep = pl.BlockSpec((1, part, width), lambda i: (0, i, 0))
    return pl.pallas_call(
        finish_kernel,
        grid=(pieces,),
        in_specs=[pl.BlockSpec(parts.shape, lambda i: (0, 0, 0)), deep] + [flat] * 4,
        out_specs=[deep] * 3,
        out_shape=[shape(1, rows, width)] * 3,
        name="finish",
    )(parts, current, z, u, w, v)


def solution(mesh):
    tile = P("layer", ("scen", "row"), "col")
    in_specs = (tile, tile, P("layer", None), tile, P(("scen", "row"), "col"))
    return jax.shard_map(local, mesh=mesh, in_specs=in_specs, out_specs=(tile,) * 3, check_vma=False)
```

```python
import jax
import jax.numpy as jnp
from jax import lax
from jax.experimental import pallas as pl
from jax.experimental.pallas import tpu as pltpu
from jax.sharding import PartitionSpec as P


via_conductance = 2.0
pad_conductance = 4.0
leakage = 0.05

SUB = 8
LANE = 128


def lanes_of(shape):
    return lax.broadcasted_iota(jnp.int32, shape, len(shape) - 1)


def rows_of(shape):
    return lax.broadcasted_iota(jnp.int32, shape, len(shape) - 2)


def turned(value, shift, axis):
    size = value.shape[axis]
    return pltpu.roll(value, shift % size, axis) if shift % size else value


def half_conductance(classes, table):
    cond = jnp.zeros(classes.shape, jnp.float32)
    for klass in range(table.shape[1]):
        cond = jnp.where(classes == klass, 0.5 * table[0, klass], cond)
    return cond


def pad_term(pads):
    return pad_conductance * pads.astype(jnp.float32) + leakage


def via_term(vias):
    return via_conductance * vias.astype(jnp.float32)


def border_rows(table, top, bottom):
    out = []
    for blocks, shifts, far in ((top, (0, 3, 5, 7), 1), (bottom, (3, 5, 7, 0), SUB - 2)):
        classes, current, pads, vias = blocks
        row = rows_of(current.shape)
        cond = half_conductance(classes, table)
        coupling = via_term(vias)
        own = pad_term(pads)
        own = jnp.where(row == far, own + coupling, own)
        parts = [turned(v, s, 0) for v, s in zip((cond, current, own, coupling), shifts)]
        out.append(
            jnp.where(row < 3, parts[0], jnp.where(row < 5, parts[1], jnp.where(row < 7, parts[2], parts[3])))
        )
    return out


def rows_kernel(table, ct, rt, pt, vt, cb, rb, pb, vb, up, down):
    up[...], down[...] = border_rows(
        table, (ct[0], rt[0], pt[0], vt[...]), (cb[0], rb[0], pb[0], vb[...])
    )


def border_columns(low, high):
    lane = lanes_of(low[0].shape)
    out = None
    for blocks, shifts, far, start in ((high, (3, 5, 7, 8), LANE - 2, 0), (low, (8, 11, 13, 15), 1, 8)):
        cond, current, own, coupling = blocks
        own = jnp.where(lane == far, own + coupling, own)
        parts = [turned(v, s, 1) for v, s in zip((cond, current, own, coupling), shifts)]
        at = lane - start
        side = jnp.where(at < 3, parts[0], jnp.where(at < 5, parts[1], jnp.where(at < 7, parts[2], parts[3])))
        out = side if out is None else jnp.where(lane < start, out, side)
    return out


def tile_kernel(table, classes, current, pads, vias, bulk, coup, strips):
    rows, width = vias.shape

    def strip(s, carry):
        at = pl.ds(pl.multiple_of(s * SUB, SUB), SUB)
        bulk[0, at, :] = half_conductance(classes[0, at, :], table)
        bulk[1, at, :] = current[0, at, :]
        bulk[2, at, :] = pad_term(pads[0, at, :])
        coup[at, :] = via_term(vias[at, :])
        return carry

    lax.fori_loop(0, rows // SUB, strip, 0)
    sides = [
        (bulk[0, :, at], bulk[1, :, at], bulk[2, :, at], coup[:, at])
        for at in (slice(0, LANE), slice(width - LANE, width))
    ]
    strips[...] = border_columns(*sides).T[: 2 * SUB]


def spread_rows(message, below):
    shifts, firsts = ((0, 5, 3, 1), (0, 0, 0, 0)) if below else ((5, 3, 1, 0), (5, 6, 6, 7))
    counts = (3, 2, 2, 1)
    row = rows_of(message.shape)
    return [
        jnp.where((row >= f) & (row < f + n), turned(message, s, 0), 0.0)
        for s, f, n in zip(shifts, firsts, counts)
    ]


def send_kernel(top, bottom, strips, send):
    width = top.shape[1]
    c = lax.axis_index("col")
    blocks = []
    for at in (slice(0, LANE), slice(width - LANE, width)):
        above = spread_rows(top[:, at], False)
        under = spread_rows(bottom[:, at], True)
        blocks.append([jnp.concatenate([a, b], axis=0) for a, b in zip(above, under)])
    around = border_columns(*blocks)
    around = jnp.concatenate([around, jnp.zeros((LANE - 2 * SUB, LANE), jnp.float32)], axis=0).T
    high = jnp.concatenate([strips[:SUB], around[:SUB]], axis=1)
    low = jnp.concatenate([strips[SUB:], around[SUB : 2 * SUB]], axis=1)
    for k in range(send.shape[0]):
        send[k] = jnp.where(k // 2 > c, high, low)


def side_lanes(left, right):
    fill = jnp.zeros((LANE - 2 * SUB, LANE), jnp.float32)
    both = jnp.concatenate([left, right, fill], axis=0).T
    lane = lanes_of(both.shape)
    out = []
    for first, before, after in ((0, 3, 3), (3, 2, 2), (5, 2, 2), (7, 1, 1)):
        low = turned(both, LANE - before - first, 1)
        high = turned(both, -SUB - first, 1)
        out.append(jnp.where(lane >= LANE - before, low, jnp.where(lane < after, high, 0.0)))
    return out


def grid_kernel(
    own, other, coup, top, bottom, frames, recv,
    z_out, u_out, w_out, v_out, sums,
    side, rim, eh, ev, inv, z, u, flux,
):
    rows, width = coup.shape
    strips = rows // SUB
    wide = width + LANE
    columns = recv.shape[0] // 2
    c, place = lax.axis_index("col"), lax.axis_index("layer")

    for layer in range(2):
        mine = place if layer == 0 else 1 - place
        left = recv[jnp.maximum(2 * (c - 1) + mine, 0)]
        left = jnp.where(c > 0, left, 0.0)
        right = recv[jnp.minimum(2 * (c + 1) + mine, 2 * columns - 1)]
        right = jnp.where(c < columns - 1, right, 0.0)
        beside = side_lanes(left[:, :LANE], right[:, :LANE])
        corner = side_lanes(left[:, LANE:], right[:, LANE:])
        above = spread_rows(top[...] if layer == 0 else frames[:SUB], False)
        under = spread_rows(bottom[...] if layer == 0 else frames[SUB:], True)
        for k in range(4 - layer):
            side[4 * layer + k] = beside[k]
            rim[4 * layer + k, 0, :, :width] = above[k]
            rim[4 * layer + k, 1, :, :width] = under[k]
            rim[4 * layer + k, 0, :, width:] = corner[k][:SUB]
            rim[4 * layer + k, 1, :, width:] = corner[k][SUB : 2 * SUB]

    row = rows_of((SUB, wide))
    first, last = row == 0, row == SUB - 1

    def at(s):
        return pl.ds(pl.multiple_of((s + 1) * SUB, SUB), SUB)

    def tile(s):
        return pl.ds(pl.multiple_of((s - 1) * SUB, SUB), SUB)

    def given(k, layer, s):
        if isinstance(s, int) and not 1 <= s <= strips:
            return rim[4 * layer + k, 0 if s == 0 else 1]
        source = coup[tile(s), :] if k == 3 else (other if layer else own)[k, tile(s), :]
        return jnp.concatenate([source, side[4 * layer + k, tile(s), :]], axis=1)

    def after(value):
        return turned(value, -1, 1)

    def before(value):
        return turned(value, 1, 1)

    def below(value, following):
        return turned(jnp.where(first, following, value), -1, 0)

    def above_of(value, preceding):
        return turned(jnp.where(last, preceding, value), 1, 0)

    def inside(a, b, edge):
        return jnp.where((a > 0.0) & (b > 0.0), edge, 0.0)

    def beyond(value, fix):
        return jnp.concatenate([value[:, : width - LANE], fix(slice(width - LANE, wide))], axis=1)

    def scale(s):
        static = isinstance(s, int)
        k = given(3, 0, s)
        for layer in range(2):
            c = given(0, layer, s)
            on = after(c)
            h = c + on
            h = beyond(h, lambda l: inside(c[:, l], on[:, l], h[:, l]))
            if static and s == strips + 1:
                v = c + turned(c, -1, 0)
            else:
                under = below(c, given(0, layer, s + 1))
                v = c + under
                if static:
                    v = inside(c, under, v)
            eh[layer, at(s), :] = h
            ev[layer, at(s), :] = v
            diagonal = h + before(h) + v + k + given(2, layer, s)
            if not static or s > 0:
                diagonal = diagonal + above_of(v, ev[layer, at(s - 1), :])
            else:
                diagonal = diagonal + turned(v, 1, 0)
            inverse = 1.0 / diagonal
            if static and not 1 <= s <= strips:
                inverse = jnp.where(c > 0.0, inverse, 0.0)
            else:
                l = slice(width, wide)
                inverse = jnp.concatenate(
                    [inverse[:, :width], jnp.where(c[:, l] > 0.0, inverse[:, l], 0.0)], axis=1
                )
            inv[layer, at(s), :] = inverse
            z[layer, at(s), :] = given(1, layer, s) * inverse

    def loop(body, carry=None):
        def step(s, t):
            found = body(s)
            return None if t is None else tuple(a + b for a, b in zip(t, found))

        return lax.fori_loop(1, strips, step, carry)

    scale(0)
    loop(scale)
    scale(strips)
    scale(strips + 1)

    def folded(value):
        parts = [value[:, i * LANE : (i + 1) * LANE] for i in range(width // LANE)]
        while len(parts) > 1:
            parts = [a + b for a, b in zip(parts[::2], parts[1::2])]
        return parts[0]

    def down_flux(field, s, layer, x):
        fv = ev[layer, at(s), :] * (x - below(x, field[layer, at(s + 1), :]))
        flux[layer] = fv
        return fv

    def image(field, s, layer, x, exchange):
        fh = eh[layer, at(s), :] * (x - after(x))
        previous = flux[layer]
        fv = down_flux(field, s, layer, x)
        return (fh - before(fh)) + (fv - above_of(fv, previous)) + (exchange + given(2, layer, s) * x)

    def second(s):
        x = [z[layer, at(s), :] for layer in range(2)]
        exchange = given(3, 0, s) * (x[0] - x[1])
        w, y = [], []
        for layer in range(2):
            w.append(image(z, s, layer, x[layer], -exchange if layer else exchange))
            y.append(w[layer] * inv[layer, at(s), :])
            u[layer, at(s), :] = y[layer]
        if isinstance(s, int) and not 1 <= s <= strips:
            return None
        z_out[tile(s), :] = x[0][:, :width]
        w_out[tile(s), :] = w[0][:, :width]
        u_out[tile(s), :] = y[0][:, :width]
        energy = folded(sum(given(1, i, s) * x[i] for i in range(2)))
        curve = folded(sum(x[i] * w[i] for i in range(2)))
        cross = folded(sum(w[i] * y[i] for i in range(2)))
        return energy, curve, cross

    zero = jnp.zeros((SUB, LANE), jnp.float32)
    flux[...] = jnp.zeros(flux.shape, jnp.float32)
    second(0)
    totals = loop(second, (zero,) * 3)
    totals = tuple(a + b for a, b in zip(totals, second(strips)))
    second(strips + 1)

    down_flux(u, 0, 0, u[0, at(0), :])

    def third(s):
        x, y = u[0, at(s), :], u[1, at(s), :]
        exchange = given(3, 0, s) * (x - y)
        v = image(u, s, 0, x, exchange)
        v_out[tile(s), :] = v[:, :width]
        dh = y - after(y)
        dv = y - below(y, u[1, at(s + 1), :])
        there = eh[1, at(s), :] * (dh * dh) + ev[1, at(s), :] * (dv * dv)
        there = there + y * (given(2, 1, s) * y - exchange)
        return (folded(x * v + there),)

    (total,) = loop(third, (zero,))
    total = total + third(strips)[0]
    lane = lanes_of((1, LANE))
    line = jnp.zeros((1, LANE), jnp.float32)
    for k, value in enumerate(totals + (total,)):
        line = jnp.where(lane == k, jnp.sum(value, axis=(0, 1), keepdims=True), line)
    sums[...] = jnp.broadcast_to(line[None], sums.shape)


def finish_kernel(parts, fields, z, u, w, v, drop, resid, worst):
    line = jnp.sum(parts[...], axis=0)
    lane = lanes_of(line.shape)
    energy, curve, cross, last = (
        jnp.sum(jnp.where(lane == k, line, 0.0), axis=1, keepdims=True) for k in range(4)
    )
    step = energy / curve
    energy_next = step * step * cross - energy
    ratio = energy_next / energy
    curve_next = curve - 2.0 * step * cross + step * step * last - ratio * ratio * curve
    step_next = energy_next / curve_next
    mixed = step_next * step
    both = step + step_next * (1.0 + ratio)
    part = drop.shape[1]
    at = pl.ds(pl.multiple_of(pl.program_id(0) * part, SUB), part)
    here = z[at, :]
    second_drop = both * here - mixed * u[at, :]
    drop[0] = second_drop
    worst[0] = jnp.maximum(step * here, second_drop)
    resid[0] = fields[1, at, :] - both * w[at, :] + mixed * v[at, :]


def local(current, node_class, class_conductance, pad_mask, via_mask):
    _, rows, width = current.shape
    n_row, n_col = lax.axis_size("row"), lax.axis_size("col")
    up_pairs = [(i, i + 1) for i in range(n_row - 1)]
    down_pairs = [(b, a) for a, b in up_pairs]
    swap = [(0, 1), (1, 0)]
    f32 = jnp.float32
    smem = pl.BlockSpec(memory_space=pltpu.SMEM)
    vmem = pl.BlockSpec(memory_space=pltpu.VMEM)

    def kept(*dims):
        return pltpu.VMEM(dims, f32)

    def here(value):
        return pltpu.with_memory_space_constraint(value, pltpu.VMEM)

    def room(mib):
        return pltpu.CompilerParams(vmem_limit_bytes=mib << 20)

    def ends(index):
        block = pl.BlockSpec((1, SUB, width), lambda i: (0, index, 0))
        return [block] * 3 + [pl.BlockSpec((SUB, width), lambda i: (index, 0))]

    fields = (node_class, current, pad_mask, via_mask)
    far = tuple(pltpu.with_memory_space_constraint(f, pltpu.HBM) for f in fields)
    up, down = pl.pallas_call(
        rows_kernel,
        grid=(1,),
        in_specs=[smem] + ends(0) + ends(rows // SUB - 1),
        out_specs=[vmem] * 2,
        out_shape=[kept(SUB, width)] * 2,
        compiler_params=room(8),
        name="border_rows",
    )(class_conductance, *far, *far)
    top = lax.ppermute(down, "row", up_pairs)
    bottom = lax.ppermute(up, "row", down_pairs)

    bulk, coup, strips = pl.pallas_call(
        tile_kernel,
        in_specs=[smem] + [vmem] * 4,
        out_specs=[vmem] * 3,
        out_shape=[kept(3, rows, width), kept(rows, width), kept(2 * SUB, LANE)],
        compiler_params=room(16),
        name="tile_fields",
    )(class_conductance, *fields)
    other = lax.ppermute(bulk, "layer", swap)

    frames = lax.ppermute(jnp.concatenate([top, bottom], axis=0), "layer", swap)
    top, bottom = here(top), here(bottom)
    send = pl.pallas_call(
        send_kernel,
        in_specs=[vmem] * 3,
        out_specs=vmem,
        out_shape=kept(2 * n_col, SUB, 2 * LANE),
        compiler_params=room(8),
        name="border_columns",
    )(top, bottom, here(strips))
    recv = lax.all_to_all(send, ("col", "layer"), 0, 0, tiled=True)

    wide = width + LANE
    pair = pltpu.VMEM((2, rows + 4 * SUB, wide), f32)
    z, u, w, v, sums = pl.pallas_call(
        grid_kernel,
        in_specs=[vmem] * 7,
        out_specs=[vmem] * 5,
        out_shape=[kept(rows, width)] * 4 + [kept(n_row * n_col, 1, LANE)],
        scratch_shapes=[
            pltpu.VMEM((7, rows, LANE), f32),
            pltpu.VMEM((7, 2, SUB, wide), f32),
        ]
        + [pair] * 5
        + [pltpu.VMEM((2, SUB, wide), f32)],
        compiler_params=room(24),
        name="grid",
    )(here(bulk), here(other), here(coup), top, bottom, here(frames), here(recv))
    parts = lax.all_to_all(sums, ("row", "col"), 0, 0, tiled=True)

    pieces = 4
    deep = pl.BlockSpec((1, rows // pieces, width), lambda i: (0, i, 0))
    return pl.pallas_call(
        finish_kernel,
        grid=(pieces,),
        in_specs=[vmem] * 6,
        out_specs=[deep] * 3,
        out_shape=[jax.ShapeDtypeStruct((1, rows, width), f32)] * 3,
        compiler_params=room(16),
        name="finish",
    )(here(parts), here(bulk), here(z), here(u), here(w), here(v))


def solution(mesh):
    tile = P("layer", ("scen", "row"), "col")
    in_specs = (tile, tile, P("layer", None), tile, P(("scen", "row"), "col"))

    return jax.shard_map(local, mesh=mesh, in_specs=in_specs, out_specs=(tile,) * 3, check_vma=False)
```

```python
import jax
import jax.numpy as jnp
from jax import lax
from jax.experimental import pallas as pl
from jax.experimental.pallas import tpu as pltpu
from jax.sharding import PartitionSpec as P


via_conductance = 2.0
pad_conductance = 4.0
leakage = 0.05

SUB = 8
LANE = 128
TOGETHER = 5


def lanes_of(shape):
    return lax.broadcasted_iota(jnp.int32, shape, len(shape) - 1)


def rows_of(shape):
    return lax.broadcasted_iota(jnp.int32, shape, len(shape) - 2)


def turned(value, shift, axis):
    size = value.shape[axis]
    return pltpu.roll(value, shift % size, axis) if shift % size else value


def half_conductance(classes, table):
    cond = jnp.zeros(classes.shape, jnp.float32)
    for klass in range(table.shape[1]):
        cond = jnp.where(classes == klass, 0.5 * table[0, klass], cond)
    return cond


def pad_term(pads):
    return pad_conductance * pads.astype(jnp.float32) + leakage


def via_term(vias):
    return via_conductance * vias.astype(jnp.float32)


def border_rows(table, top, bottom):
    out = []
    for blocks, shifts, far in ((top, (0, 3, 5, 7), 1), (bottom, (3, 5, 7, 0), SUB - 2)):
        classes, current, pads, vias = blocks
        row = rows_of(current.shape)
        cond = half_conductance(classes, table)
        coupling = via_term(vias)
        own = pad_term(pads)
        own = jnp.where(row == far, own + coupling, own)
        parts = [turned(v, s, 0) for v, s in zip((cond, current, own, coupling), shifts)]
        out.append(
            jnp.where(row < 3, parts[0], jnp.where(row < 5, parts[1], jnp.where(row < 7, parts[2], parts[3])))
        )
    return out


def rows_kernel(table, ct, rt, pt, vt, cb, rb, pb, vb, up, down):
    up[...], down[...] = border_rows(
        table, (ct[0], rt[0], pt[0], vt[...]), (cb[0], rb[0], pb[0], vb[...])
    )


def border_columns(low, high):
    lane = lanes_of(low[0].shape)
    out = None
    for blocks, shifts, far, start in ((high, (3, 5, 7, 8), LANE - 2, 0), (low, (8, 11, 13, 15), 1, 8)):
        cond, current, own, coupling = blocks
        own = jnp.where(lane == far, own + coupling, own)
        parts = [turned(v, s, 1) for v, s in zip((cond, current, own, coupling), shifts)]
        at = lane - start
        side = jnp.where(at < 3, parts[0], jnp.where(at < 5, parts[1], jnp.where(at < 7, parts[2], parts[3])))
        out = side if out is None else jnp.where(lane < start, out, side)
    return out


def tile_kernel(table, classes, current, pads, vias, bulk, coup, strips):
    rows, width = vias.shape
    fields = [bulk.at[pl.ds(k * rows, rows)] for k in range(3)]

    def strip(s, carry):
        at = pl.ds(pl.multiple_of(s * SUB, SUB), SUB)
        fields[0][at, :] = half_conductance(classes[0, at, :], table)
        fields[1][at, :] = current[0, at, :]
        fields[2][at, :] = pad_term(pads[0, at, :])
        coup[at, :] = via_term(vias[at, :])
        return carry

    lax.fori_loop(0, rows // SUB, strip, 0)
    sides = [
        tuple(field[:, at] for field in fields) + (coup[:, at],)
        for at in (slice(0, LANE), slice(width - LANE, width))
    ]
    strips[...] = border_columns(*sides).T[: 2 * SUB]


def spread_rows(message, below):
    shifts, firsts = ((0, 5, 3, 1), (0, 0, 0, 0)) if below else ((5, 3, 1, 0), (5, 6, 6, 7))
    counts = (3, 2, 2, 1)
    row = rows_of(message.shape)
    return [
        jnp.where((row >= f) & (row < f + n), turned(message, s, 0), 0.0)
        for s, f, n in zip(shifts, firsts, counts)
    ]


def send_kernel(top, bottom, strips, send):
    width = top.shape[1]
    c = lax.axis_index("col")
    blocks = []
    for at in (slice(0, LANE), slice(width - LANE, width)):
        above = spread_rows(top[:, at], False)
        under = spread_rows(bottom[:, at], True)
        blocks.append([jnp.concatenate([a, b], axis=0) for a, b in zip(above, under)])
    around = border_columns(*blocks)
    around = jnp.concatenate([around, jnp.zeros((LANE - 2 * SUB, LANE), jnp.float32)], axis=0).T
    high = jnp.concatenate([strips[:SUB], around[:SUB]], axis=1)
    low = jnp.concatenate([strips[SUB:], around[SUB : 2 * SUB]], axis=1)
    for k in range(send.shape[0]):
        send[k] = jnp.where(k // 2 > c, high, low)


def side_lanes(left, right):
    fill = jnp.zeros((LANE - 2 * SUB, LANE), jnp.float32)
    both = jnp.concatenate([left, right, fill], axis=0).T
    lane = lanes_of(both.shape)
    out = []
    for first, before, after in ((0, 3, 3), (3, 2, 2), (5, 2, 2), (7, 1, 1)):
        low = turned(both, LANE - before - first, 1)
        high = turned(both, -SUB - first, 1)
        out.append(jnp.where(lane >= LANE - before, low, jnp.where(lane < after, high, 0.0)))
    return out


def grid_kernel(
    own, other, coup, recv,
    z_out, u_out, w_out, v_out, sums,
    side, rim, eh, el, ev, inv, z, u,
):
    rows, width = coup.shape
    strips = rows // SUB
    wide = width + LANE
    columns = recv.shape[0] // 2
    c, place = lax.axis_index("col"), lax.axis_index("layer")

    for layer in range(2):
        mine = place if layer == 0 else 1 - place
        left = recv[jnp.maximum(2 * (c - 1) + mine, 0)]
        left = jnp.where(c > 0, left, 0.0)
        right = recv[jnp.minimum(2 * (c + 1) + mine, 2 * columns - 1)]
        right = jnp.where(c < columns - 1, right, 0.0)
        beside = side_lanes(left[:, :LANE], right[:, :LANE])
        corner = side_lanes(left[:, LANE:], right[:, LANE:])
        source = other if layer else own
        above = spread_rows(source[3 * rows : 3 * rows + SUB], False)
        under = spread_rows(source[3 * rows + SUB :], True)
        for k in range(4 - layer):
            side[4 * layer + k] = beside[k]
            rim[4 * layer + k, 0, :, :width] = above[k]
            rim[4 * layer + k, 1, :, :width] = under[k]
            rim[4 * layer + k, 0, :, width:] = corner[k][:SUB]
            rim[4 * layer + k, 1, :, width:] = corner[k][SUB : 2 * SUB]

    row = rows_of((SUB, wide))
    first, last = row == 0, row == SUB - 1

    def at(s):
        return pl.ds(pl.multiple_of((s + 1) * SUB, SUB), SUB)

    def tile(s, k=0):
        return pl.ds(pl.multiple_of(k * rows + (s - 1) * SUB, SUB), SUB)

    def given(k, layer, s):
        if isinstance(s, int) and not 1 <= s <= strips:
            return rim[4 * layer + k, 0 if s == 0 else 1]
        source = coup[tile(s), :] if k == 3 else (other if layer else own)[tile(s, k), :]
        return jnp.concatenate([source, side[4 * layer + k, tile(s), :]], axis=1)

    def after(value):
        return turned(value, -1, 1)

    def before(value):
        return turned(value, 1, 1)

    def below(value, following):
        return turned(jnp.where(first, following, value), -1, 0)

    def above_of(value, preceding):
        return turned(jnp.where(last, preceding, value), 1, 0)

    def inside(a, b, edge):
        return jnp.where((a > 0.0) & (b > 0.0), edge, 0.0)

    def seam(value, blocks, fix):
        parts, start = [], 0
        for k in sorted(blocks):
            parts += [value[:, start : k * LANE]] if k * LANE > start else []
            parts.append(fix(slice(k * LANE, (k + 1) * LANE)))
            start = (k + 1) * LANE
        return jnp.concatenate(parts + ([value[:, start:]] if start < wide else []), axis=1)

    end = width // LANE

    def scale(s, previous):
        static = isinstance(s, int)
        k = given(3, 0, s)
        kept = []
        for layer in range(2):
            c = given(0, layer, s)
            on, back = after(c), before(c)
            h, g = c + on, c + back
            h = seam(h, (end - 1, end), lambda l: inside(c[:, l], on[:, l], h[:, l]))
            g = seam(g, (0, end), lambda l: inside(c[:, l], back[:, l], g[:, l]))
            if static and s == strips + 1:
                v = c + turned(c, -1, 0)
            else:
                under = below(c, given(0, layer, s + 1))
                v = c + under
                if static:
                    v = inside(c, under, v)
            eh[layer, at(s), :] = h
            el[layer, at(s), :] = g
            ev[layer, at(s), :] = v
            prior = v if previous is None else previous[layer]
            diagonal = ((h + g) + (v + above_of(v, prior))) + (k + given(2, layer, s))
            inverse = 1.0 / diagonal
            if static and not 1 <= s <= strips:
                inverse = jnp.where(c > 0.0, inverse, 0.0)
            else:
                inverse = seam(inverse, (end,), lambda l: jnp.where(c[:, l] > 0.0, inverse[:, l], 0.0))
            inv[layer, at(s), :] = inverse
            z[layer, at(s), :] = given(1, layer, s) * inverse
            kept.append(v)
        return kept, None

    def loop(body, recall, totals=()):
        def step(i, totals):
            s = 1 + i * TOGETHER
            previous = recall(s - 1)
            for k in range(TOGETHER):
                previous, found = body(s + k, previous)
                totals = tuple(a + b for a, b in zip(totals, found or ()))
            return totals

        return lax.fori_loop(0, (strips - 1) // TOGETHER, step, totals)

    def edge_above(s):
        return [ev[layer, at(s), :] for layer in range(2)]

    scale(0, None)
    loop(scale, edge_above)
    kept, _ = scale(strips, edge_above(strips - 1))
    scale(strips + 1, kept)

    def folded(value):
        parts = [value[:, i * LANE : (i + 1) * LANE] for i in range(width // LANE)]
        while len(parts) > 1:
            parts = [a + b for a, b in zip(parts[::2], parts[1::2])]
        return parts[0]

    def down_flux(field, s, layer):
        x = field[layer, at(s), :]
        return ev[layer, at(s), :] * (x - below(x, field[layer, at(s + 1), :]))

    def image(field, s, layer, x, exchange, previous):
        across = eh[layer, at(s), :] * (x - after(x)) + el[layer, at(s), :] * (x - before(x))
        fv = down_flux(field, s, layer)
        return across + (fv - above_of(fv, previous)) + (exchange + given(2, layer, s) * x), fv

    def second(s, previous):
        x = [z[layer, at(s), :] for layer in range(2)]
        exchange = given(3, 0, s) * (x[0] - x[1])
        w, y, kept = [], [], []
        for layer in range(2):
            found, fv = image(z, s, layer, x[layer], -exchange if layer else exchange, previous[layer])
            w.append(found)
            kept.append(fv)
            y.append(found * inv[layer, at(s), :])
            u[layer, at(s), :] = y[layer]
        if isinstance(s, int) and not 1 <= s <= strips:
            return kept, None
        z_out[tile(s), :] = x[0][:, :width]
        w_out[tile(s), :] = w[0][:, :width]
        u_out[tile(s), :] = y[0][:, :width]
        energy = folded(sum(given(1, i, s) * x[i] for i in range(2)))
        curve = folded(sum(x[i] * w[i] for i in range(2)))
        cross = folded(sum(w[i] * y[i] for i in range(2)))
        return kept, (energy, curve, cross)

    def flux_above(field):
        return lambda s: [down_flux(field, s, layer) for layer in range(2)]

    zero = jnp.zeros((SUB, LANE), jnp.float32)
    nothing = jnp.zeros((SUB, wide), jnp.float32)
    second(0, [nothing] * 2)
    totals = loop(second, flux_above(z), (zero,) * 3)
    kept, found = second(strips, flux_above(z)(strips - 1))
    totals = tuple(a + b for a, b in zip(totals, found))
    second(strips + 1, kept)

    def third(s, previous):
        x, y = u[0, at(s), :], u[1, at(s), :]
        exchange = given(3, 0, s) * (x - y)
        v, fv = image(u, s, 0, x, exchange, previous)
        v_out[tile(s), :] = v[:, :width]
        dh = y - after(y)
        dv = y - below(y, u[1, at(s + 1), :])
        there = eh[1, at(s), :] * (dh * dh) + ev[1, at(s), :] * (dv * dv)
        there = there + y * (given(2, 1, s) * y - exchange)
        return fv, (folded(x * v + there),)

    (total,) = loop(third, lambda s: down_flux(u, s, 0), (zero,))
    total = total + third(strips, down_flux(u, strips - 1, 0))[1][0]
    lane = lanes_of((1, LANE))
    line = jnp.zeros((1, LANE), jnp.float32)
    for k, value in enumerate(totals + (total,)):
        line = jnp.where(lane == k, jnp.sum(value, axis=(0, 1), keepdims=True), line)
    sums[...] = jnp.broadcast_to(line[None], sums.shape)


def finish_kernel(parts, fields, z, u, w, v, drop, resid, worst, steps):
    rows, part = z.shape[0], drop.shape[1]

    @pl.when(pl.program_id(0) == 0)
    def _():
        line = jnp.sum(parts[...], axis=0)
        lane = lanes_of(line.shape)
        energy, curve, cross, last = (
            jnp.sum(jnp.where(lane == k, line, 0.0), axis=1, keepdims=True) for k in range(4)
        )
        step = energy / curve
        energy_next = step * step * cross - energy
        ratio = energy_next / energy
        curve_next = curve - 2.0 * step * cross + step * step * last - ratio * ratio * curve
        step_next = energy_next / curve_next
        for k, value in enumerate((step, step + step_next * (1.0 + ratio), step_next * step)):
            steps[k] = jnp.broadcast_to(value, steps.shape[1:])

    step, both, mixed = (steps[k, :1, :1] for k in range(3))
    at = pl.ds(pl.multiple_of(pl.program_id(0) * part, SUB), part)
    here = z[at, :]
    second_drop = both * here - mixed * u[at, :]
    drop[0] = second_drop
    worst[0] = jnp.maximum(step * here, second_drop)
    given = fields[pl.ds(pl.multiple_of(rows + pl.program_id(0) * part, SUB), part), :]
    resid[0] = given - both * w[at, :] + mixed * v[at, :]


def local(current, node_class, class_conductance, pad_mask, via_mask):
    _, rows, width = current.shape
    n_row, n_col = lax.axis_size("row"), lax.axis_size("col")
    up_pairs = [(i, i + 1) for i in range(n_row - 1)]
    down_pairs = [(b, a) for a, b in up_pairs]
    swap = [(0, 1), (1, 0)]
    f32 = jnp.float32
    smem = pl.BlockSpec(memory_space=pltpu.SMEM)
    vmem = pl.BlockSpec(memory_space=pltpu.VMEM)

    def kept(*dims):
        return pltpu.VMEM(dims, f32)

    def here(value):
        return pltpu.with_memory_space_constraint(value, pltpu.VMEM)

    def room(mib):
        return pltpu.CompilerParams(vmem_limit_bytes=mib << 20)

    def ends(index):
        block = pl.BlockSpec((1, SUB, width), lambda i: (0, index, 0))
        return [block] * 3 + [pl.BlockSpec((SUB, width), lambda i: (index, 0))]

    fields = (node_class, current, pad_mask, via_mask)
    far = tuple(pltpu.with_memory_space_constraint(f, pltpu.HBM) for f in fields)
    up, down = pl.pallas_call(
        rows_kernel,
        grid=(1,),
        in_specs=[smem] + ends(0) + ends(rows // SUB - 1),
        out_specs=[vmem] * 2,
        out_shape=[kept(SUB, width)] * 2,
        compiler_params=room(8),
        name="border_rows",
    )(pltpu.with_memory_space_constraint(class_conductance, pltpu.HBM), *far, *far)
    top = lax.ppermute(down, "row", up_pairs)
    bottom = lax.ppermute(up, "row", down_pairs)

    bulk, coup, strips = pl.pallas_call(
        tile_kernel,
        in_specs=[smem] + [vmem] * 4,
        out_specs=[vmem] * 3,
        out_shape=[kept(3 * rows + 2 * SUB, width), kept(rows, width), kept(2 * SUB, LANE)],
        compiler_params=room(16),
        name="tile_fields",
    )(class_conductance, *fields)
    bulk = lax.dynamic_update_slice(bulk, top, (3 * rows, 0))
    bulk = lax.dynamic_update_slice(bulk, bottom, (3 * rows + SUB, 0))
    send = pl.pallas_call(
        send_kernel,
        in_specs=[vmem] * 3,
        out_specs=vmem,
        out_shape=kept(2 * n_col, SUB, 2 * LANE),
        compiler_params=room(8),
        name="border_columns",
    )(here(top), here(bottom), here(strips))
    other = lax.ppermute(bulk, "layer", swap)
    recv = lax.all_to_all(send, ("col", "layer"), 0, 0, tiled=True)

    wide = width + LANE
    pair = pltpu.VMEM((2, rows + 4 * SUB, wide), f32)
    z, u, w, v, sums = pl.pallas_call(
        grid_kernel,
        in_specs=[vmem] * 4,
        out_specs=[vmem] * 5,
        out_shape=[kept(rows, width)] * 4 + [kept(n_row * n_col, 1, LANE)],
        scratch_shapes=[
            pltpu.VMEM((7, rows, LANE), f32),
            pltpu.VMEM((7, 2, SUB, wide), f32),
        ]
        + [pair] * 6,
        compiler_params=room(28),
        name="grid",
    )(here(bulk), here(other), here(coup), here(recv))
    parts = lax.all_to_all(sums, ("row", "col"), 0, 0, tiled=True)

    pieces = 2
    deep = pl.BlockSpec((1, rows // pieces, width), lambda i: (0, i, 0))
    return pl.pallas_call(
        finish_kernel,
        grid=(pieces,),
        in_specs=[vmem] * 6,
        out_specs=[deep] * 3,
        out_shape=[jax.ShapeDtypeStruct((1, rows, width), f32)] * 3,
        scratch_shapes=[pltpu.VMEM((3, SUB, LANE), f32)],
        compiler_params=room(16),
        name="finish",
    )(here(parts), here(bulk), here(z), here(u), here(w), here(v))


def solution(mesh):
    tile = P("layer", ("scen", "row"), "col")
    in_specs = (tile, tile, P("layer", None), tile, P(("scen", "row"), "col"))

    return jax.shard_map(local, mesh=mesh, in_specs=in_specs, out_specs=(tile,) * 3, check_vma=False)
```

```python
import jax
import jax.numpy as jnp
from jax import lax
from jax.experimental import pallas as pl
from jax.experimental.pallas import tpu as pltpu
from jax.sharding import PartitionSpec as P


via_conductance = 2.0
pad_conductance = 4.0
leakage = 0.05

SUB = 8
LANE = 128


def lanes_of(shape):
    return lax.broadcasted_iota(jnp.int32, shape, len(shape) - 1)


def rows_of(shape):
    return lax.broadcasted_iota(jnp.int32, shape, len(shape) - 2)


def turned(value, shift, axis):
    size = value.shape[axis]
    return pltpu.roll(value, shift % size, axis) if shift % size else value


def half_conductance(classes, table):
    cond = jnp.zeros(classes.shape, jnp.float32)
    for klass in range(table.shape[1]):
        cond = jnp.where(classes == klass, 0.5 * table[0, klass], cond)
    return cond


def pad_term(pads):
    return pad_conductance * pads.astype(jnp.float32) + leakage


def via_term(vias):
    return via_conductance * vias.astype(jnp.float32)


def border_rows(table, top, bottom):
    out = []
    for blocks, shifts, far in ((top, (0, 3, 5, 7), 1), (bottom, (3, 5, 7, 0), SUB - 2)):
        classes, current, pads, vias = blocks
        row = rows_of(current.shape)
        cond = half_conductance(classes, table)
        coupling = via_term(vias)
        own = pad_term(pads)
        own = jnp.where(row == far, own + coupling, own)
        parts = [turned(v, s, 0) for v, s in zip((cond, current, own, coupling), shifts)]
        out.append(
            jnp.where(row < 3, parts[0], jnp.where(row < 5, parts[1], jnp.where(row < 7, parts[2], parts[3])))
        )
    return out


def rows_kernel(table, ct, rt, pt, vt, cb, rb, pb, vb, up, down):
    up[...], down[...] = border_rows(
        table, (ct[0], rt[0], pt[0], vt[...]), (cb[0], rb[0], pb[0], vb[...])
    )


def border_columns(low, high):
    lane = lanes_of(low[0].shape)
    out = None
    for blocks, shifts, far, start in ((high, (3, 5, 7, 8), LANE - 2, 0), (low, (8, 11, 13, 15), 1, 8)):
        cond, current, own, coupling = blocks
        own = jnp.where(lane == far, own + coupling, own)
        parts = [turned(v, s, 1) for v, s in zip((cond, current, own, coupling), shifts)]
        at = lane - start
        side = jnp.where(at < 3, parts[0], jnp.where(at < 5, parts[1], jnp.where(at < 7, parts[2], parts[3])))
        out = side if out is None else jnp.where(lane < start, out, side)
    return out


def tile_kernel(table, classes, current, pads, vias, bulk, coup, strips):
    rows, width = vias.shape
    fields = [bulk.at[pl.ds(k * rows, rows)] for k in range(3)]

    def strip(s, carry):
        at = pl.ds(pl.multiple_of(s * SUB, SUB), SUB)
        fields[0][at, :] = half_conductance(classes[0, at, :], table)
        fields[1][at, :] = current[0, at, :]
        fields[2][at, :] = pad_term(pads[0, at, :])
        coup[at, :] = via_term(vias[at, :])
        return carry

    lax.fori_loop(0, rows // SUB, strip, 0)
    sides = [
        tuple(field[:, at] for field in fields) + (coup[:, at],)
        for at in (slice(0, LANE), slice(width - LANE, width))
    ]
    strips[...] = border_columns(*sides).T[: 2 * SUB]


def spread_rows(message, below):
    shifts, firsts = ((0, 5, 3, 1), (0, 0, 0, 0)) if below else ((5, 3, 1, 0), (5, 6, 6, 7))
    counts = (3, 2, 2, 1)
    row = rows_of(message.shape)
    return [
        jnp.where((row >= f) & (row < f + n), turned(message, s, 0), 0.0)
        for s, f, n in zip(shifts, firsts, counts)
    ]


def send_kernel(top, bottom, strips, send):
    width = top.shape[1]
    c = lax.axis_index("col")
    blocks = []
    for at in (slice(0, LANE), slice(width - LANE, width)):
        above = spread_rows(top[:, at], False)
        under = spread_rows(bottom[:, at], True)
        blocks.append([jnp.concatenate([a, b], axis=0) for a, b in zip(above, under)])
    around = border_columns(*blocks)
    around = jnp.concatenate([around, jnp.zeros((LANE - 2 * SUB, LANE), jnp.float32)], axis=0).T
    high = jnp.concatenate([strips[:SUB], around[:SUB]], axis=1)
    low = jnp.concatenate([strips[SUB:], around[SUB : 2 * SUB]], axis=1)
    for k in range(send.shape[0]):
        send[k] = jnp.where(k // 2 > c, high, low)


def side_lanes(left, right, rows=LANE):
    fill = jnp.zeros((LANE - 2 * SUB, LANE), jnp.float32)
    both = jnp.concatenate([left, right, fill], axis=0).T[:rows]
    lane = lanes_of(both.shape)
    out = []
    for first, before, after in ((0, 3, 3), (3, 2, 2), (5, 2, 2), (7, 1, 1)):
        low = turned(both, LANE - before - first, 1)
        high = turned(both, -SUB - first, 1)
        out.append(jnp.where(lane >= LANE - before, low, jnp.where(lane < after, high, 0.0)))
    return out


def grid_kernel(
    own, other, coup, recv,
    z, u, w_out, v_out, sums,
    side, rim, eh, el, ev, inv,
):
    rows, width = coup.shape
    strips = rows // SUB
    wide = width + LANE
    columns = recv.shape[0] // 2
    c, place = lax.axis_index("col"), lax.axis_index("layer")

    for layer in range(2):
        mine = place if layer == 0 else 1 - place
        left = recv[jnp.maximum(2 * (c - 1) + mine, 0)]
        left = jnp.where(c > 0, left, 0.0)
        right = recv[jnp.minimum(2 * (c + 1) + mine, 2 * columns - 1)]
        right = jnp.where(c < columns - 1, right, 0.0)
        beside = side_lanes(left[:, :LANE], right[:, :LANE])
        corner = side_lanes(left[:, LANE:], right[:, LANE:], 2 * SUB)
        source = other if layer else own
        above = spread_rows(source[3 * rows : 3 * rows + SUB], False)
        under = spread_rows(source[3 * rows + SUB :], True)
        for k in range(4 - layer):
            side[4 * layer + k] = beside[k]
            rim[4 * layer + k, 0, :, :width] = above[k]
            rim[4 * layer + k, 1, :, :width] = under[k]
            rim[4 * layer + k, 0, :, width:] = corner[k][:SUB]
            rim[4 * layer + k, 1, :, width:] = corner[k][SUB:]

    row = rows_of((SUB, wide))
    first, last = row == 0, row == SUB - 1

    def at(s):
        return pl.ds((s + 1) * SUB, SUB)

    def tile(s, k=0):
        return pl.ds(k * rows + (s - 1) * SUB, SUB)

    def given(k, layer, s):
        if not 1 <= s <= strips:
            return rim[4 * layer + k, 0 if s == 0 else 1]
        source = coup[tile(s), :] if k == 3 else (other if layer else own)[tile(s, k), :]
        return jnp.concatenate([source, side[4 * layer + k, tile(s), :]], axis=1)

    def after(value):
        return turned(value, -1, 1)

    def before(value):
        return turned(value, 1, 1)

    def below(value, following):
        return turned(jnp.where(first, following, value), -1, 0)

    def above_of(value, preceding):
        return turned(jnp.where(last, preceding, value), 1, 0)

    def inside(a, b, edge):
        return jnp.where((a > 0.0) & (b > 0.0), edge, 0.0)

    def seam(value, blocks, fix):
        parts, start = [], 0
        for k in sorted(blocks):
            parts += [value[:, start : k * LANE]] if k * LANE > start else []
            parts.append(fix(slice(k * LANE, (k + 1) * LANE)))
            start = (k + 1) * LANE
        return jnp.concatenate(parts + ([value[:, start:]] if start < wide else []), axis=1)

    end = width // LANE

    def scale(s, previous):
        k = given(3, 0, s)
        kept = []
        for layer in range(2):
            c = given(0, layer, s)
            on, back = after(c), before(c)
            h, g = c + on, c + back
            h = seam(h, (end - 1, end), lambda l: inside(c[:, l], on[:, l], h[:, l]))
            g = seam(g, (0, end), lambda l: inside(c[:, l], back[:, l], g[:, l]))
            if s == strips + 1:
                v = c + turned(c, -1, 0)
            else:
                under = below(c, given(0, layer, s + 1))
                v = c + under
                if s in (0, strips):
                    v = inside(c, under, v)
            eh[layer, at(s), :] = h
            el[layer, at(s), :] = g
            ev[layer, at(s), :] = v
            prior = v if previous is None else previous[layer]
            diagonal = ((h + g) + (v + above_of(v, prior))) + (k + given(2, layer, s))
            inverse = 1.0 / diagonal
            if not 1 <= s <= strips:
                inverse = jnp.where(c > 0.0, inverse, 0.0)
            else:
                inverse = seam(inverse, (end,), lambda l: jnp.where(c[:, l] > 0.0, inverse[:, l], 0.0))
            inv[layer, at(s), :] = inverse
            z[layer, at(s), :] = given(1, layer, s) * inverse
            kept.append(v)
        return kept

    kept = None
    for s in range(strips + 2):
        kept = scale(s, kept)

    def folded(value):
        parts = [value[:, i * LANE : (i + 1) * LANE] for i in range(width // LANE)]
        while len(parts) > 1:
            parts = [a + b for a, b in zip(parts[::2], parts[1::2])]
        return parts[0]

    def down_flux(field, s, layer):
        x = field[layer, at(s), :]
        return ev[layer, at(s), :] * (x - below(x, field[layer, at(s + 1), :]))

    def image(field, s, layer, x, exchange, previous):
        across = eh[layer, at(s), :] * (x - after(x)) + el[layer, at(s), :] * (x - before(x))
        fv = down_flux(field, s, layer)
        return across + (fv - above_of(fv, previous)) + (exchange + given(2, layer, s) * x), fv

    def second(s, previous):
        x = [z[layer, at(s), :] for layer in range(2)]
        exchange = given(3, 0, s) * (x[0] - x[1])
        w, y, kept = [], [], []
        for layer in range(2):
            found, fv = image(z, s, layer, x[layer], -exchange if layer else exchange, previous[layer])
            w.append(found)
            kept.append(fv)
            y.append(found * inv[layer, at(s), :])
            u[layer, at(s), :] = y[layer]
        if not 1 <= s <= strips:
            return kept, None
        w_out[tile(s), :] = w[0][:, :width]
        energy = folded(sum(given(1, i, s) * x[i] for i in range(2)))
        curve = folded(sum(x[i] * w[i] for i in range(2)))
        cross = folded(sum(w[i] * y[i] for i in range(2)))
        return kept, (energy, curve, cross)

    zero = jnp.zeros((SUB, LANE), jnp.float32)
    kept, totals = [jnp.zeros((SUB, wide), jnp.float32)] * 2, (zero,) * 3
    for s in range(strips + 2):
        kept, found = second(s, kept)
        totals = tuple(a + b for a, b in zip(totals, found)) if found else totals

    def third(s, previous):
        x, y = u[0, at(s), :], u[1, at(s), :]
        exchange = given(3, 0, s) * (x - y)
        v, fv = image(u, s, 0, x, exchange, previous)
        v_out[tile(s), :] = v[:, :width]
        dh = y - after(y)
        dv = y - below(y, u[1, at(s + 1), :])
        there = eh[1, at(s), :] * (dh * dh) + ev[1, at(s), :] * (dv * dv)
        there = there + y * (given(2, 1, s) * y - exchange)
        return fv, folded(x * v + there)

    kept, total = down_flux(u, 0, 0), zero
    for s in range(1, strips + 1):
        kept, found = third(s, kept)
        total = total + found
    lane = lanes_of((1, LANE))
    line = jnp.zeros((1, LANE), jnp.float32)
    for k, value in enumerate(totals + (total,)):
        line = jnp.where(lane == k, jnp.sum(value, axis=(0, 1), keepdims=True), line)
    sums[...] = jnp.broadcast_to(line[None], sums.shape)


def finish_kernel(parts, fields, z, u, w, v, drop, resid, worst, steps):
    rows, width = w.shape
    part = drop.shape[1]

    @pl.when(pl.program_id(0) == 0)
    def _():
        line = jnp.sum(parts[...], axis=0)
        lane = lanes_of(line.shape)
        energy, curve, cross, last = (
            jnp.sum(jnp.where(lane == k, line, 0.0), axis=1, keepdims=True) for k in range(4)
        )
        step = energy / curve
        energy_next = step * step * cross - energy
        ratio = energy_next / energy
        curve_next = curve - 2.0 * step * cross + step * step * last - ratio * ratio * curve
        step_next = energy_next / curve_next
        for k, value in enumerate((step, step + step_next * (1.0 + ratio), step_next * step)):
            steps[k] = jnp.broadcast_to(value, steps.shape[1:])

    step, both, mixed = (steps[k, :1, :1] for k in range(3))
    at = pl.ds(pl.multiple_of(pl.program_id(0) * part, SUB), part)
    inner = pl.ds(pl.multiple_of(2 * SUB + pl.program_id(0) * part, SUB), part)
    here = z[0, inner, :width]
    second_drop = both * here - mixed * u[0, inner, :width]
    drop[0] = second_drop
    worst[0] = jnp.maximum(step * here, second_drop)
    given = fields[pl.ds(pl.multiple_of(rows + pl.program_id(0) * part, SUB), part), :]
    resid[0] = given - both * w[at, :] + mixed * v[at, :]


def local(current, node_class, class_conductance, pad_mask, via_mask):
    _, rows, width = current.shape
    n_row, n_col = lax.axis_size("row"), lax.axis_size("col")
    up_pairs = [(i, i + 1) for i in range(n_row - 1)]
    down_pairs = [(b, a) for a, b in up_pairs]
    swap = [(0, 1), (1, 0)]
    f32 = jnp.float32
    smem = pl.BlockSpec(memory_space=pltpu.SMEM)
    vmem = pl.BlockSpec(memory_space=pltpu.VMEM)

    def kept(*dims):
        return pltpu.VMEM(dims, f32)

    def here(value):
        return pltpu.with_memory_space_constraint(value, pltpu.VMEM)

    def room(mib):
        return pltpu.CompilerParams(vmem_limit_bytes=mib << 20)

    def ends(index):
        block = pl.BlockSpec((1, SUB, width), lambda i: (0, index, 0))
        return [block] * 3 + [pl.BlockSpec((SUB, width), lambda i: (index, 0))]

    fields = (node_class, current, pad_mask, via_mask)
    far = tuple(pltpu.with_memory_space_constraint(f, pltpu.HBM) for f in fields)
    up, down = pl.pallas_call(
        rows_kernel,
        grid=(1,),
        in_specs=[smem] + ends(0) + ends(rows // SUB - 1),
        out_specs=[vmem] * 2,
        out_shape=[kept(SUB, width)] * 2,
        compiler_params=room(8),
        name="border_rows",
    )(pltpu.with_memory_space_constraint(class_conductance, pltpu.HBM), *far, *far)
    top = lax.ppermute(down, "row", up_pairs)
    bottom = lax.ppermute(up, "row", down_pairs)

    bulk, coup, strips = pl.pallas_call(
        tile_kernel,
        in_specs=[smem] + [vmem] * 4,
        out_specs=[vmem] * 3,
        out_shape=[kept(3 * rows + 2 * SUB, width), kept(rows, width), kept(2 * SUB, LANE)],
        compiler_params=room(16),
        name="tile_fields",
    )(class_conductance, *fields)
    bulk = lax.dynamic_update_slice(bulk, top, (3 * rows, 0))
    bulk = lax.dynamic_update_slice(bulk, bottom, (3 * rows + SUB, 0))
    send = pl.pallas_call(
        send_kernel,
        in_specs=[vmem] * 3,
        out_specs=vmem,
        out_shape=kept(2 * n_col, SUB, 2 * LANE),
        compiler_params=room(8),
        name="border_columns",
    )(here(top), here(bottom), here(strips))
    other = lax.ppermute(bulk, "layer", swap)
    recv = lax.all_to_all(send, ("col", "layer"), 0, 0, tiled=True)

    wide = width + LANE
    pair = kept(2, rows + 4 * SUB, wide)
    z, u, w, v, sums = pl.pallas_call(
        grid_kernel,
        in_specs=[vmem] * 4,
        out_specs=[vmem] * 5,
        out_shape=[pair] * 2 + [kept(rows, width)] * 2 + [kept(n_row * n_col, 1, LANE)],
        scratch_shapes=[
            pltpu.VMEM((7, rows, LANE), f32),
            pltpu.VMEM((7, 2, SUB, wide), f32),
        ]
        + [pair] * 4,
        compiler_params=room(28),
        name="grid",
    )(here(bulk), here(other), here(coup), here(recv))
    heart = 3 * n_row // 4
    order = [heart] + [i for i in range(n_row) if i != heart]
    group = [i * n_col + k for i in order for k in range(n_col)]
    parts = lax.all_to_all(sums, ("row", "col"), 0, 0, axis_index_groups=[group], tiled=True)

    pieces = 2
    deep = pl.BlockSpec((1, rows // pieces, width), lambda i: (0, i, 0))
    return pl.pallas_call(
        finish_kernel,
        grid=(pieces,),
        in_specs=[vmem] * 6,
        out_specs=[deep] * 3,
        out_shape=[jax.ShapeDtypeStruct((1, rows, width), f32)] * 3,
        scratch_shapes=[pltpu.VMEM((3, SUB, LANE), f32)],
        compiler_params=room(16),
        name="finish",
    )(here(parts), here(bulk), here(z), here(u), here(w), here(v))


def solution(mesh):
    tile = P("layer", ("scen", "row"), "col")
    in_specs = (tile, tile, P("layer", None), tile, P(("scen", "row"), "col"))

    return jax.shard_map(local, mesh=mesh, in_specs=in_specs, out_specs=(tile,) * 3, check_vma=False)
```

```python
import jax
import jax.numpy as jnp
from jax import lax
from jax.experimental import pallas as pl
from jax.experimental.pallas import tpu as pltpu
from jax.sharding import PartitionSpec as P


via_conductance = 2.0
pad_conductance = 4.0
leakage = 0.05

SUB = 8
TURN = 2
LANE = 128


def lanes_of(shape):
    return lax.broadcasted_iota(jnp.int32, shape, len(shape) - 1)


def rows_of(shape):
    return lax.broadcasted_iota(jnp.int32, shape, len(shape) - 2)


def turned(value, shift, axis):
    size = value.shape[axis]
    return pltpu.roll(value, shift % size, axis) if shift % size else value


def half_conductance(classes, table):
    cond = jnp.zeros(classes.shape, jnp.float32)
    for klass in range(table.shape[1]):
        cond = jnp.where(classes == klass, 0.5 * table[0, klass], cond)
    return cond


def pad_term(pads):
    return pad_conductance * pads.astype(jnp.float32) + leakage


def via_term(vias):
    return via_conductance * vias.astype(jnp.float32)


def border_rows(table, top, bottom):
    out = []
    for blocks, shifts, far in ((top, (0, 3, 5, 7), 1), (bottom, (3, 5, 7, 0), SUB - 2)):
        classes, current, pads, vias = blocks
        row = rows_of(current.shape)
        cond = half_conductance(classes, table)
        coupling = via_term(vias)
        own = pad_term(pads)
        own = jnp.where(row == far, own + coupling, own)
        parts = [turned(v, s, 0) for v, s in zip((cond, current, own, coupling), shifts)]
        out.append(
            jnp.where(row < 3, parts[0], jnp.where(row < 5, parts[1], jnp.where(row < 7, parts[2], parts[3])))
        )
    return out


def rows_kernel(table, ct, rt, pt, vt, cb, rb, pb, vb, up, down):
    up[...], down[...] = border_rows(
        table, (ct[0], rt[0], pt[0], vt[...]), (cb[0], rb[0], pb[0], vb[...])
    )


def border_columns(low, high):
    lane = lanes_of(low[0].shape)
    out = None
    for blocks, shifts, far, start in ((high, (3, 5, 7, 8), LANE - 2, 0), (low, (8, 11, 13, 15), 1, 8)):
        cond, current, own, coupling = blocks
        own = jnp.where(lane == far, own + coupling, own)
        parts = [turned(v, s, 1) for v, s in zip((cond, current, own, coupling), shifts)]
        at = lane - start
        side = jnp.where(at < 3, parts[0], jnp.where(at < 5, parts[1], jnp.where(at < 7, parts[2], parts[3])))
        out = side if out is None else jnp.where(lane < start, out, side)
    return out


def tile_kernel(table, classes, current, pads, vias, bulk, coup, strips):
    rows, width = vias.shape
    fields = [bulk.at[pl.ds(k * rows, rows)] for k in range(3)]

    for s in range(rows // SUB):
        at = pl.ds(s * SUB, SUB)
        fields[0][at, :] = half_conductance(classes[0, at, :], table)
        fields[1][at, :] = current[0, at, :]
        fields[2][at, :] = pad_term(pads[0, at, :])
        coup[at, :] = via_term(vias[at, :])
    sides = [
        tuple(field[:, at] for field in fields) + (coup[:, at],)
        for at in (slice(0, LANE), slice(width - LANE, width))
    ]
    strips[...] = border_columns(*sides).T[: 2 * SUB]


def spread_rows(message, below):
    shifts, firsts = ((0, 5, 3, 1), (0, 0, 0, 0)) if below else ((5, 3, 1, 0), (5, 6, 6, 7))
    counts = (3, 2, 2, 1)
    row = rows_of(message.shape)
    return [
        jnp.where((row >= f) & (row < f + n), turned(message, s, 0), 0.0)
        for s, f, n in zip(shifts, firsts, counts)
    ]


def send_kernel(top, bottom, strips, send):
    width = top.shape[1]
    c = lax.axis_index("col")
    blocks = []
    for at in (slice(0, LANE), slice(width - LANE, width)):
        above = spread_rows(top[:, at], False)
        under = spread_rows(bottom[:, at], True)
        blocks.append([jnp.concatenate([a, b], axis=0) for a, b in zip(above, under)])
    around = border_columns(*blocks)
    around = jnp.concatenate([around, jnp.zeros((LANE - 2 * SUB, LANE), jnp.float32)], axis=0).T
    high = jnp.concatenate([strips[:SUB], around[:SUB]], axis=1)
    low = jnp.concatenate([strips[SUB:], around[SUB : 2 * SUB]], axis=1)
    count = send.shape[0] // 2
    for k in range(2 * count):
        send[k] = jnp.where((k // 2 + TURN) % count > c, high, low)


def side_lanes(left, right, rows=LANE):
    fill = jnp.zeros((LANE - 2 * SUB, LANE), jnp.float32)
    both = jnp.concatenate([left, right, fill], axis=0).T[:rows]
    lane = lanes_of(both.shape)
    out = []
    for first, before, after in ((0, 3, 3), (3, 2, 2), (5, 2, 2), (7, 1, 1)):
        low = turned(both, LANE - before - first, 1)
        high = turned(both, -SUB - first, 1)
        out.append(jnp.where(lane >= LANE - before, low, jnp.where(lane < after, high, 0.0)))
    return out


def grid_kernel(
    own, other, coup, recv,
    z, u, w_out, v_out, sums,
    side, rim, eh, el, ev, inv,
):
    rows, width = coup.shape
    strips = rows // SUB
    wide = width + LANE
    columns = recv.shape[0] // 2
    c, place = lax.axis_index("col"), lax.axis_index("layer")

    for layer in range(2):
        mine = place if layer == 0 else 1 - place
        left = recv[2 * lax.rem(c - 1 - TURN + 4 * columns, columns) + mine]
        left = jnp.where(c > 0, left, 0.0)
        right = recv[2 * lax.rem(c + 1 - TURN + 4 * columns, columns) + mine]
        right = jnp.where(c < columns - 1, right, 0.0)
        beside = side_lanes(left[:, :LANE], right[:, :LANE])
        corner = side_lanes(left[:, LANE:], right[:, LANE:], 2 * SUB)
        source = other if layer else own
        above = spread_rows(source[3 * rows : 3 * rows + SUB], False)
        under = spread_rows(source[3 * rows + SUB :], True)
        for k in range(4 - layer):
            side[4 * layer + k] = beside[k]
            rim[4 * layer + k, 0, :, :width] = above[k]
            rim[4 * layer + k, 1, :, :width] = under[k]
            rim[4 * layer + k, 0, :, width:] = corner[k][:SUB]
            rim[4 * layer + k, 1, :, width:] = corner[k][SUB:]

    row = rows_of((SUB, wide))
    first, last = row == 0, row == SUB - 1

    def at(s):
        return pl.ds((s + 1) * SUB, SUB)

    def tile(s, k=0):
        return pl.ds(k * rows + (s - 1) * SUB, SUB)

    def given(k, layer, s):
        if not 1 <= s <= strips:
            return rim[4 * layer + k, 0 if s == 0 else 1]
        source = coup[tile(s), :] if k == 3 else (other if layer else own)[tile(s, k), :]
        return jnp.concatenate([source, side[4 * layer + k, tile(s), :]], axis=1)

    def after(value):
        return turned(value, -1, 1)

    def before(value):
        return turned(value, 1, 1)

    def below(value, following):
        return turned(jnp.where(first, following, value), -1, 0)

    def above_of(value, preceding):
        return turned(jnp.where(last, preceding, value), 1, 0)

    def inside(a, b, edge):
        return jnp.where((a > 0.0) & (b > 0.0), edge, 0.0)

    def seam(value, blocks, fix):
        parts, start = [], 0
        for k in sorted(blocks):
            parts += [value[:, start : k * LANE]] if k * LANE > start else []
            parts.append(fix(slice(k * LANE, (k + 1) * LANE)))
            start = (k + 1) * LANE
        return jnp.concatenate(parts + ([value[:, start:]] if start < wide else []), axis=1)

    end = width // LANE

    def scale(s, previous):
        k = given(3, 0, s)
        kept = []
        for layer in range(2):
            c = given(0, layer, s)
            on, back = after(c), before(c)
            h, g = c + on, c + back
            h = seam(h, (end - 1, end), lambda l: inside(c[:, l], on[:, l], h[:, l]))
            g = seam(g, (0, end), lambda l: inside(c[:, l], back[:, l], g[:, l]))
            if s == strips + 1:
                v = c + turned(c, -1, 0)
            else:
                under = below(c, given(0, layer, s + 1))
                v = c + under
                if s in (0, strips):
                    v = inside(c, under, v)
            eh[layer, at(s), :] = h
            el[layer, at(s), :] = g
            ev[layer, at(s), :] = v
            prior = v if previous is None else previous[layer]
            diagonal = ((h + g) + (v + above_of(v, prior))) + (k + given(2, layer, s))
            inverse = 1.0 / diagonal
            if not 1 <= s <= strips:
                inverse = jnp.where(c > 0.0, inverse, 0.0)
            else:
                inverse = seam(inverse, (end,), lambda l: jnp.where(c[:, l] > 0.0, inverse[:, l], 0.0))
            inv[layer, at(s), :] = inverse
            z[layer, at(s), :] = given(1, layer, s) * inverse
            kept.append(v)
        return kept

    kept = None
    for s in range(strips + 2):
        kept = scale(s, kept)

    def folded(value):
        parts = [value[:, i * LANE : (i + 1) * LANE] for i in range(width // LANE)]
        while len(parts) > 1:
            parts = [a + b for a, b in zip(parts[::2], parts[1::2])]
        return parts[0]

    def down_flux(field, s, layer):
        x = field[layer, at(s), :]
        return ev[layer, at(s), :] * (x - below(x, field[layer, at(s + 1), :]))

    def image(field, s, layer, x, exchange, previous):
        across = eh[layer, at(s), :] * (x - after(x)) + el[layer, at(s), :] * (x - before(x))
        fv = down_flux(field, s, layer)
        return across + (fv - above_of(fv, previous)) + (exchange + given(2, layer, s) * x), fv

    def second(s, previous):
        x = [z[layer, at(s), :] for layer in range(2)]
        exchange = given(3, 0, s) * (x[0] - x[1])
        w, y, kept = [], [], []
        for layer in range(2):
            found, fv = image(z, s, layer, x[layer], -exchange if layer else exchange, previous[layer])
            w.append(found)
            kept.append(fv)
            y.append(found * inv[layer, at(s), :])
            u[layer, at(s), :] = y[layer]
        if not 1 <= s <= strips:
            return kept, None
        w_out[tile(s), :] = w[0][:, :width]
        energy = folded(sum(given(1, i, s) * x[i] for i in range(2)))
        curve = folded(sum(x[i] * w[i] for i in range(2)))
        cross = folded(sum(w[i] * y[i] for i in range(2)))
        return kept, (energy, curve, cross)

    zero = jnp.zeros((SUB, LANE), jnp.float32)
    kept, totals = [jnp.zeros((SUB, wide), jnp.float32)] * 2, (zero,) * 3
    for s in range(strips + 2):
        kept, found = second(s, kept)
        totals = tuple(a + b for a, b in zip(totals, found)) if found else totals

    def third(s, previous):
        x, y = u[0, at(s), :], u[1, at(s), :]
        exchange = given(3, 0, s) * (x - y)
        v, fv = image(u, s, 0, x, exchange, previous)
        v_out[tile(s), :] = v[:, :width]
        dh = y - after(y)
        dv = y - below(y, u[1, at(s + 1), :])
        there = eh[1, at(s), :] * (dh * dh) + ev[1, at(s), :] * (dv * dv)
        there = there + y * (given(2, 1, s) * y - exchange)
        return fv, folded(x * v + there)

    kept, total = down_flux(u, 0, 0), zero
    for s in range(1, strips + 1):
        kept, found = third(s, kept)
        total = total + found
    lane = lanes_of((1, LANE))
    line = jnp.zeros((1, LANE), jnp.float32)
    for k, value in enumerate(totals + (total,)):
        line = jnp.where(lane == k, jnp.sum(value, axis=(0, 1), keepdims=True), line)
    sums[...] = jnp.broadcast_to(line[None], sums.shape)


def finish_kernel(parts, fields, z, u, w, v, drop, resid, worst, steps):
    rows, width = w.shape
    part = drop.shape[1]

    @pl.when(pl.program_id(0) == 0)
    def _():
        line = jnp.sum(parts[...], axis=0)
        lane = lanes_of(line.shape)
        energy, curve, cross, last = (
            jnp.sum(jnp.where(lane == k, line, 0.0), axis=1, keepdims=True) for k in range(4)
        )
        step = energy / curve
        energy_next = step * step * cross - energy
        ratio = energy_next / energy
        curve_next = curve - 2.0 * step * cross + step * step * last - ratio * ratio * curve
        step_next = energy_next / curve_next
        for k, value in enumerate((step, step + step_next * (1.0 + ratio), step_next * step)):
            steps[k] = jnp.broadcast_to(value, steps.shape[1:])

    step, both, mixed = (steps[k, :1, :1] for k in range(3))
    at = pl.ds(pl.multiple_of(pl.program_id(0) * part, SUB), part)
    inner = pl.ds(pl.multiple_of(2 * SUB + pl.program_id(0) * part, SUB), part)
    here = z[0, inner, :width]
    second_drop = both * here - mixed * u[0, inner, :width]
    drop[0] = second_drop
    worst[0] = jnp.maximum(step * here, second_drop)
    given = fields[pl.ds(pl.multiple_of(rows + pl.program_id(0) * part, SUB), part), :]
    resid[0] = given - both * w[at, :] + mixed * v[at, :]


def local(current, node_class, class_conductance, pad_mask, via_mask):
    _, rows, width = current.shape
    n_row, n_col = lax.axis_size("row"), lax.axis_size("col")
    up_pairs = [(i, i + 1) for i in range(n_row - 1)]
    down_pairs = [(b, a) for a, b in up_pairs]
    swap = [(0, 1), (1, 0)]
    f32 = jnp.float32
    smem = pl.BlockSpec(memory_space=pltpu.SMEM)
    vmem = pl.BlockSpec(memory_space=pltpu.VMEM)

    def kept(*dims):
        return pltpu.VMEM(dims, f32)

    def here(value):
        return pltpu.with_memory_space_constraint(value, pltpu.VMEM)

    def room(mib):
        return pltpu.CompilerParams(vmem_limit_bytes=mib << 20)

    def ends(index):
        block = pl.BlockSpec((1, SUB, width), lambda i: (0, index, 0))
        return [block] * 3 + [pl.BlockSpec((SUB, width), lambda i: (index, 0))]

    fields = (node_class, current, pad_mask, via_mask)
    far = tuple(pltpu.with_memory_space_constraint(f, pltpu.HBM) for f in fields)
    up, down = pl.pallas_call(
        rows_kernel,
        grid=(1,),
        in_specs=[smem] + ends(0) + ends(rows // SUB - 1),
        out_specs=[vmem] * 2,
        out_shape=[kept(SUB, width)] * 2,
        compiler_params=room(8),
        name="border_rows",
    )(pltpu.with_memory_space_constraint(class_conductance, pltpu.HBM), *far, *far)
    bottom = lax.ppermute(up, "row", down_pairs)
    top = lax.ppermute(down, "row", up_pairs)

    bulk, coup, strips = pl.pallas_call(
        tile_kernel,
        in_specs=[smem] + [vmem] * 4,
        out_specs=[vmem] * 3,
        out_shape=[kept(3 * rows + 2 * SUB, width), kept(rows, width), kept(2 * SUB, LANE)],
        compiler_params=room(16),
        name="tile_fields",
    )(class_conductance, *fields)
    bulk = lax.dynamic_update_slice(bulk, top, (3 * rows, 0))
    bulk = lax.dynamic_update_slice(bulk, bottom, (3 * rows + SUB, 0))
    send = pl.pallas_call(
        send_kernel,
        in_specs=[vmem] * 3,
        out_specs=vmem,
        out_shape=kept(2 * n_col, SUB, 2 * LANE),
        compiler_params=room(8),
        name="border_columns",
    )(here(top), here(bottom), here(strips))
    other = lax.ppermute(bulk, "layer", swap)
    line = [2 * ((i + TURN) % n_col) + k for i in range(n_col) for k in range(2)]
    recv = lax.all_to_all(send, ("col", "layer"), 0, 0, axis_index_groups=[line], tiled=True)

    wide = width + LANE
    pair = kept(2, rows + 4 * SUB, wide)
    z, u, w, v, sums = pl.pallas_call(
        grid_kernel,
        in_specs=[vmem] * 4,
        out_specs=[vmem] * 5,
        out_shape=[pair] * 2 + [kept(rows, width)] * 2 + [kept(n_row * n_col, 1, LANE)],
        scratch_shapes=[
            pltpu.VMEM((7, rows, LANE), f32),
            pltpu.VMEM((7, 2, SUB, wide), f32),
        ]
        + [pair] * 4,
        compiler_params=room(28),
        name="grid",
    )(here(bulk), here(other), here(coup), here(recv))
    heart = 13 * n_row // 16
    order = [heart] + [i for i in range(n_row) if i != heart]
    group = [i * n_col + (k + TURN) % n_col for i in order for k in range(n_col)]
    parts = lax.all_to_all(sums, ("row", "col"), 0, 0, axis_index_groups=[group], tiled=True)

    pieces = 2
    deep = pl.BlockSpec((1, rows // pieces, width), lambda i: (0, i, 0))
    return pl.pallas_call(
        finish_kernel,
        grid=(pieces,),
        in_specs=[vmem] * 6,
        out_specs=[deep] * 3,
        out_shape=[jax.ShapeDtypeStruct((1, rows, width), f32)] * 3,
        scratch_shapes=[pltpu.VMEM((3, SUB, LANE), f32)],
        compiler_params=room(16),
        name="finish",
    )(here(parts), here(bulk), here(z), here(u), here(w), here(v))


def solution(mesh):
    tile = P("layer", ("scen", "row"), "col")
    in_specs = (tile, tile, P("layer", None), tile, P(("scen", "row"), "col"))

    return jax.shard_map(local, mesh=mesh, in_specs=in_specs, out_specs=(tile,) * 3, check_vma=False)
```
